8 devices in a mesh: fsdp: 8 (over z, y, x, core).
Axes of the slice: x: 2, y: 2, z: 1, core: 2. Of those that a mesh axis runs over, the one named last changes fastest.
Arguments:
- left_mat: bfloat16 [49152, 2560], P('fsdp')
- right_mat: bfloat16 [2560, 2560], P('fsdp')
Outputs:
- output: bfloat16 [49152, 2560], P('fsdp')
All inputs are finite; a program needn't handle non-finite values.
Results may differ from the reference program's by a relative error of at most 0.001.
Values are sent between devices in bfloat16 or wider.
A program may use at most 1 GiB of HBM per device.

```python
import jax
import jax.numpy as jnp

ROWS_TOTAL = 49152
IN_WIDTH = 2560
OUT_WIDTH = 2560


def setup_inputs(seed: int = 0) -> dict:
    base_key = jax.random.key(seed)
    key_left, key_right = jax.random.split(base_key)
    left_vals = jax.random.normal(key_left, (ROWS_TOTAL, IN_WIDTH), jnp.float32)
    right_vals = jax.random.normal(key_right, (IN_WIDTH, OUT_WIDTH), jnp.float32) * (IN_WIDTH ** -0.5)
    return {"left_mat": left_vals.astype(jnp.bfloat16), "right_mat": right_vals.astype(jnp.bfloat16)}


def reference(left_mat, right_mat):
    return jnp.dot(left_mat, right_mat, preferred_element_type=jnp.float32).astype(jnp.bfloat16)
```

```python
import jax
import jax.numpy as jnp
from jax import lax
from jax.experimental import pallas as pl
from jax.experimental.pallas import tpu as pltpu
from jax.sharding import PartitionSpec as P

MESH = pl.DeviceIdType.MESH
BF16 = jnp.bfloat16
F32 = jnp.float32
ROWS = 6144
SLAB = 1024
SLABS = ROWS // SLAB
TRIP = 3 * SLAB
DEPTH = 2560
KT = 256
PW = 256
PANELS = 10
BLK = 320
HALF = BLK // 2
PART = 128
FIRST = 7
ACCP = 3
GRANT = int(21.4 * 2**20)


def _place():
    me = lax.axis_index("fsdp")
    core = me % 2
    x = (me // 2) % 2
    y = me // 4
    return me, core, x, y


def _ktiles():
    _, _, x, y = _place()
    own, other = 5 * y, 5 * (1 - y)
    return (
        [own + 3 * x + i for i in range(2)]
        + [own + 2 * (1 - x) + i for i in range(3)]
        + [other + 3 * x + i for i in range(2)]
        + [other + 2 * (1 - x) + i for i in range(3)]
    )


class Mxu:
    def __init__(self, accs, abuf, bbuf):
        self.accs, self.abuf, self.bbuf = accs, abuf, bbuf
        self.kt = _ktiles()

    def acc(self, rng, q, p):
        return self.accs[(rng * 2 + q) * 4 + p]

    def push(self, panel, i, reg):
        rows = pl.ds(pl.multiple_of(self.kt[i] * KT, KT), KT)
        for q in range(2):
            pltpu.matmul_push_rhs(self.bbuf[panel, rows, :], staging_register=reg, mxu_index=q)

    def drop(self, reg):
        zero = jnp.zeros((PART, KT), BF16)
        for q in range(2):
            pltpu.matmul_acc_lhs(self.acc(0, q, 0), zero, load_staged_rhs=reg)

    def clear(self):
        for r in self.accs:
            pltpu.matmul_pop(r)

    def tile(self, rng, slab, panel, nextpanel, poss, start_reg, emit):
        n = len(poss)
        reg = start_reg
        pieces = [(p, q) for p in range(4) for q in range(2)]
        slots = 4 if n > 4 else n - 1
        per = -(-len(pieces) // max(slots, 1))
        for k, i in enumerate(poss):
            for q in range(2):
                for p in range(4):
                    rows = pl.ds(pl.multiple_of(slab * SLAB + q * 512 + p * PART, PART), PART)
                    pltpu.matmul_acc_lhs(
                        self.acc(rng, q, p), self.abuf[i, rows, :], load_staged_rhs=reg if p == 0 else None
                    )
            reg = 1 - reg
            if k < n - 1:
                self.push(panel, poss[k + 1], reg)
            else:
                self.push(nextpanel, poss[0], reg)
            if k >= 1:
                for p, q in pieces[(k - 1) * per : k * per]:
                    emit(q * 512 + p * PART, pltpu.matmul_pop(self.acc(1 - rng, q, p)))
        return reg

    def drain(self, rng, emit):
        for p in range(4):
            for q in range(2):
                emit(q * 512 + p * PART, pltpu.matmul_pop(self.acc(rng, q, p)))


def _kernel1(a_ref, b_ref, abuf, bbuf, c1_ref, psum, stage, asem, bsem, osem, ssem, rsem, psem):
    me, core, x, y = _place()
    xn = 4 * y + 2 * (1 - x) + core
    yn = 4 * (1 - y) + 2 * x + core
    dn = 4 * (1 - y) + 2 * (1 - x) + core
    other = 4 * y + 2 * x + (1 - core)
    oxn = 4 * y + 2 * (1 - x) + (1 - core)
    oyn = 4 * (1 - y) + 2 * x + (1 - core)
    odn = 4 * (1 - y) + 2 * (1 - x) + (1 - core)
    kt = _ktiles()

    def rows(dev, part=0, size=BLK):
        return pl.ds(pl.multiple_of(dev * BLK + part * HALF, 32), size)

    def remote(kind, n, sl, dev):
        piece = bbuf.at[n, sl]
        return pltpu.make_async_remote_copy(
            src_ref=piece, dst_ref=piece, send_sem=ssem.at[kind, n], recv_sem=rsem.at[kind, n],
            device_id=(dev,), device_id_type=MESH,
        )

    send = {
        0: lambda n: remote(0, n, rows(me), xn),
        1: lambda n: remote(1, n, rows(me), yn),
        2: lambda n: remote(2, n, rows(xn, 0, HALF), yn),
        3: lambda n: remote(3, n, rows(yn, 1, HALF), xn),
        4: lambda n: remote(4, n, rows(xn), other),
        5: lambda n: remote(5, n, rows(yn), other),
        6: lambda n: remote(6, n, rows(dn), other),
    }
    recv = {
        0: lambda n: remote(0, n, rows(xn), xn),
        1: lambda n: remote(1, n, rows(yn), yn),
        2: lambda n: remote(2, n, rows(dn, 0, HALF), yn),
        3: lambda n: remote(3, n, rows(dn, 1, HALF), xn),
        4: lambda n: remote(4, n, rows(oxn), other),
        5: lambda n: remote(5, n, rows(oyn), other),
        6: lambda n: remote(6, n, rows(odn), other),
    }

    def pair(part, dev):
        lo, size = ((0, ACCP), (ACCP, PANELS - ACCP))[part]
        piece = bbuf.at[pl.ds(lo, size), rows(dev)]
        return pltpu.make_async_remote_copy(
            src_ref=piece, dst_ref=piece, send_sem=psem.at[0, part], recv_sem=psem.at[1, part],
            device_id=(other,), device_id_type=MESH,
        )

    def aload(i):
        cols = pl.ds(pl.multiple_of(kt[i] * KT, KT), KT)
        return pltpu.make_async_copy(a_ref.at[:, cols], abuf.at[i], asem.at[i])

    def bload(n):
        return pltpu.make_async_copy(b_ref.at[:, pl.ds(n * PW, PW)], bbuf.at[n, rows(me)], bsem.at[n])

    def arrived(n):
        recv[0](n).wait_recv()
        recv[1](n).wait_recv()
        for kind in (2, 3, 4, 5):
            send[kind](n).start()

    def ahead(n):
        send[0](n).start()
        send[1](n).start()

    def diagonal(n):
        recv[2](n).wait_recv()
        recv[3](n).wait_recv()
        send[6](n).start()

    def service1(n):
        arrived(n)
        ahead(n + 2)

    def xy_ready(n):
        recv[4](n).wait_recv()
        recv[5](n).wait_recv()

    def d_ready(n):
        recv[6](n).wait_recv()

    def product(n, row, poss):
        total = None
        for i in poss:
            left = abuf[i, pl.ds(pl.multiple_of(row, SLAB), SLAB), :]
            right = bbuf[n, pl.ds(pl.multiple_of(kt[i] * KT, KT), KT), :]
            part = jnp.dot(left, right, preferred_element_type=F32)
            total = part if total is None else total + part
        return total

    def out_copy(g, panel, t):
        return pltpu.make_async_copy(
            stage.at[g % 2], c1_ref.at[panel, pl.ds(pl.multiple_of(t * TRIP, TRIP), TRIP)], osem.at[g % 2]
        )

    def keep(n, poss, slot, t, add=False):
        for s in range(3):
            row = t * TRIP + s * SLAB
            at = slice(s * SLAB, (s + 1) * SLAB)
            value = product(n, row, poss)
            psum[slot, at, :] = psum[slot, at, :] + value if add else value

    def final(n, poss, slot, t):
        g = 2 * n + t

        @pl.when(g >= 2)
        def _():
            out_copy(g, 0, 0).wait()

        for s in range(3):
            row = t * TRIP + s * SLAB
            value = product(n, row, poss)
            if slot is not None:
                value = psum[slot, s * SLAB : (s + 1) * SLAB, :] + value
            stage[g % 2, s * SLAB : (s + 1) * SLAB, :] = value.astype(BF16)
        out_copy(g, n, t).start()

    def halves(body, between=None):
        def trip(t, _):
            if between is not None:
                pl.when(t == 1)(between)
            body(t)
            return 0

        lax.fori_loop(0, 2, trip, 0)

    for n in range(PANELS):
        bload(n).start()
    for i in range(2):
        aload(i).start()
    barrier = pltpu.get_barrier_semaphore()
    for dev in (other, xn, yn):
        pl.semaphore_signal(barrier, inc=1, device_id=(dev,), device_id_type=MESH)
    pl.semaphore_wait(barrier, 3)
    bload(0).wait()
    ahead(0)
    bload(1).wait()
    bload(2).wait()
    pair(0, me).start()
    ahead(1)
    for n in range(3, PANELS):
        bload(n).wait()
    pair(1, me).start()

    own, mid, far = [0, 1], [2, 3, 4, 5, 6], [7, 8, 9]
    aload(0).wait()
    aload(1).wait()
    for i in range(2, 10):
        aload(i).start()
    pair(0, other).wait_recv()

    def own_half(v, _):
        @pl.when(v == 4)
        def _():
            service1(0)

        keep(v // 2, own, v, v % 2)
        return 0

    lax.fori_loop(0, 5, own_half, 0)
    for i in range(2, 7):
        aload(i).wait()
    xy_ready(0)
    halves(lambda t: keep(0, mid, t, t, True))
    service1(1)
    diagonal(0)
    xy_ready(1)
    halves(lambda t: keep(1, mid, 2 + t, t, True))
    service1(2)
    for i in range(7, 10):
        aload(i).wait()
    d_ready(0)
    halves(lambda t: final(0, far, t, t))
    diagonal(1)
    xy_ready(2)
    keep(2, mid, 4, 0, True)
    service1(3)
    d_ready(1)
    halves(lambda t: final(1, far, 2 + t, t), lambda: diagonal(2))
    d_ready(2)
    final(2, far, 4, 0)
    final(2, own + mid + far, None, 1)
    service1(4)
    xy_ready(3)
    pair(1, other).wait_recv()
    halves(lambda t: keep(3, own + mid, t, t), lambda: diagonal(3))
    service1(5)
    d_ready(3)
    halves(lambda t: final(3, far, t, t), lambda: diagonal(4))

    def full_half(u, _):
        n, t = 4 + u // 2, u % 2

        @pl.when(t == 0)
        def _():
            xy_ready(n)
            d_ready(n)

        @pl.when((u >= 1) & (u <= 2))
        def _():
            service1(5 + u)
            diagonal(4 + u)

        @pl.when(u == 3)
        def _():
            arrived(8)

        @pl.when(u == 4)
        def _():
            diagonal(7)

        @pl.when(u == 5)
        def _():
            arrived(9)
            diagonal(8)

        final(n, own + mid + far, None, t)
        return 0

    lax.fori_loop(0, 2 * (FIRST - 4), full_half, 0)
    diagonal(9)
    for n in range(FIRST, PANELS):
        xy_ready(n)
        d_ready(n)
    for kind in range(7):
        for n in range(PANELS):
            send[kind](n).wait_send()
    for part in range(2):
        pair(part, me).wait_send()
    for g in range(2):
        out_copy(g, 0, 0).wait()


def _kernel2(abuf, bbuf, c1_ref, c_ref, stage, move, osem, lsem, wsem, *accs):
    mxu = Mxu(accs, abuf, bbuf)
    trips = (PANELS - FIRST) * SLABS // 2
    poss = list(range(10))

    def load(u):
        return pltpu.make_async_copy(c1_ref.at[u], move.at[u % 3], lsem.at[u % 3])

    def store(u):
        cols = pl.ds(pl.multiple_of(u * PW, PW), PW)
        return pltpu.make_async_copy(move.at[u % 3], c_ref.at[:, cols], wsem.at[u % 3])

    def out_copy(tau):
        panel = FIRST + tau // SLABS
        return pltpu.make_async_copy(
            stage.at[tau % 4],
            c_ref.at[
                pl.ds(pl.multiple_of((tau % SLABS) * SLAB, SLAB), SLAB), pl.ds(pl.multiple_of(panel * PW, PW), PW)
            ],
            osem.at[tau % 4],
        )

    load(0).start()
    mxu.clear()
    mxu.push(FIRST, 0, 0)

    def trip(u, _):
        @pl.when((u >= 1) & (u <= FIRST))
        def _():
            load(u - 1).wait()
            store(u - 1).start()

        @pl.when((u >= 3) & (u <= FIRST + 2))
        def _():
            store(u - 3).wait()

        @pl.when((u >= 1) & (u < FIRST))
        def _():
            load(u).start()

        for j in range(2):
            tau = 2 * u + j - 1

            @pl.when(tau >= 4)
            def _():
                out_copy(tau - 4).wait()

        reg = 0
        for j in range(2):
            tau = 2 * u + j
            panel = FIRST + tau // SLABS
            nextpanel = FIRST + ((tau + 1) // SLABS) % (PANELS - FIRST)

            def emit(row, value, slot=(tau + 3) % 4):
                stage[slot, pl.ds(row, PART), :] = value.astype(BF16)

            reg = mxu.tile(j, tau % SLABS, panel, nextpanel, poss, reg, emit)

        @pl.when(u > 0)
        def _():
            out_copy(2 * u - 1).start()

        out_copy(2 * u).start()
        return 0

    lax.fori_loop(0, trips, trip, 0)
    last = 2 * trips - 1
    out_copy(last - 4).wait()

    def emit(row, value):
        stage[last % 4, pl.ds(row, PART), :] = value.astype(BF16)

    mxu.drain(1, emit)
    out_copy(last).start()
    mxu.drop(0)
    for u in range(trips - 3, FIRST):
        store(u).wait()
    for tau in range(last - 3, last + 1):
        out_copy(tau).wait()


def _with_accs(kernel):
    def run(*refs):
        specs = [pltpu.ACC(q)((PART, PW), F32) for _ in range(2) for q in range(2) for _ in range(4)]
        pl.run_scoped(lambda *accs: kernel(*refs, *accs), *specs)

    return run


def _local(a, b):
    any_ = pl.BlockSpec(memory_space=pltpu.HBM)
    vmem = pl.BlockSpec(memory_space=pltpu.VMEM)
    dma = pltpu.SemaphoreType.DMA
    abuf, bbuf, c1 = pl.pallas_call(
        _kernel1,
        out_shape=(
            pltpu.VMEM((10, ROWS, KT), BF16),
            pltpu.VMEM((PANELS, DEPTH, PW), BF16),
            pltpu.HBM((FIRST, ROWS, PW), BF16),
        ),
        in_specs=[any_, any_],
        out_specs=(vmem, vmem, any_),
        scratch_shapes=[
            pltpu.VMEM((5, TRIP, PW), F32),
            pltpu.VMEM((2, TRIP, PW), BF16),
            dma((10,)),
            dma((PANELS,)),
            dma((2,)),
            dma((7, PANELS)),
            dma((7, PANELS)),
            dma((2, 2)),
        ],
        compiler_params=pltpu.CompilerParams(
            collective_id=0, has_side_effects=True, vmem_limit_bytes=GRANT
        ),
    )(a, b)
    abuf = pltpu.with_memory_space_constraint(abuf, pltpu.VMEM)
    bbuf = pltpu.with_memory_space_constraint(bbuf, pltpu.VMEM)
    c1 = pltpu.with_memory_space_constraint(c1, pltpu.HBM)
    return pl.pallas_call(
        _with_accs(_kernel2),
        out_shape=jax.ShapeDtypeStruct((ROWS, DEPTH), BF16),
        in_specs=[vmem, vmem, any_],
        out_specs=any_,
        scratch_shapes=[
            pltpu.VMEM((4, SLAB, PW), BF16),
            pltpu.VMEM((3, ROWS, PW), BF16),
            dma((4,)),
            dma((3,)),
            dma((3,)),
        ],
        compiler_params=pltpu.CompilerParams(vmem_limit_bytes=GRANT),
    )(abuf, bbuf, c1)


def solution(mesh):
    spec = P("fsdp", None)
    return jax.shard_map(_local, mesh=mesh, in_specs=(spec, spec), out_specs=spec, check_vma=False)
```

```python
import jax
import jax.numpy as jnp
from jax import lax
from jax.experimental import pallas as pl
from jax.experimental.pallas import tpu as pltpu
from jax.sharding import PartitionSpec as P

MESH = pl.DeviceIdType.MESH
BF16 = jnp.bfloat16
F32 = jnp.float32
ROWS = 6144
SLAB = 1024
SLABS = ROWS // SLAB
TRIP = 3 * SLAB
DEPTH = 2560
KT = 256
PW = 256
PANELS = 10
BLK = 320
HALF = BLK // 2
PART = 128
FIRST = 7
GRANT = int(21.4 * 2**20)


def _place():
    me = lax.axis_index("fsdp")
    core = me % 2
    x = (me // 2) % 2
    y = me // 4
    return me, core, x, y


def _ktiles():
    _, _, x, y = _place()
    own, other = 5 * y, 5 * (1 - y)
    return (
        [own + 3 * x + i for i in range(2)]
        + [own + 2 * (1 - x) + i for i in range(3)]
        + [other + 3 * x + i for i in range(2)]
        + [other + 2 * (1 - x) + i for i in range(3)]
    )


class Mxu:
    def __init__(self, accs, abuf, bbuf):
        self.accs, self.abuf, self.bbuf = accs, abuf, bbuf
        self.kt = _ktiles()

    def acc(self, rng, q, p):
        return self.accs[(rng * 2 + q) * 4 + p]

    def push(self, panel, i, reg):
        rows = pl.ds(pl.multiple_of(self.kt[i] * KT, KT), KT)
        for q in range(2):
            pltpu.matmul_push_rhs(self.bbuf[panel, rows, :], staging_register=reg, mxu_index=q)

    def drop(self, reg):
        zero = jnp.zeros((PART, KT), BF16)
        for q in range(2):
            pltpu.matmul_acc_lhs(self.acc(0, q, 0), zero, load_staged_rhs=reg)

    def clear(self):
        for r in self.accs:
            pltpu.matmul_pop(r)

    def tile(self, rng, slab, panel, nextpanel, poss, start_reg, emit):
        n = len(poss)
        reg = start_reg
        pieces = [(p, q) for p in range(4) for q in range(2)]
        slots = 4 if n > 4 else n - 1
        per = -(-len(pieces) // max(slots, 1))
        for k, i in enumerate(poss):
            for q in range(2):
                for p in range(4):
                    rows = pl.ds(pl.multiple_of(slab * SLAB + q * 512 + p * PART, PART), PART)
                    pltpu.matmul_acc_lhs(
                        self.acc(rng, q, p), self.abuf[i, rows, :], load_staged_rhs=reg if p == 0 else None
                    )
            reg = 1 - reg
            if k < n - 1:
                self.push(panel, poss[k + 1], reg)
            else:
                self.push(nextpanel, poss[0], reg)
            if k >= 1:
                for p, q in pieces[(k - 1) * per : k * per]:
                    emit(q * 512 + p * PART, pltpu.matmul_pop(self.acc(1 - rng, q, p)))
        return reg

    def drain(self, rng, emit):
        for p in range(4):
            for q in range(2):
                emit(q * 512 + p * PART, pltpu.matmul_pop(self.acc(rng, q, p)))


def _kernel1(a_ref, b_ref, abuf, bbuf, c1_ref, psum, stage, asem, bsem, osem, ssem, rsem, psem):
    me, core, x, y = _place()
    xn = 4 * y + 2 * (1 - x) + core
    yn = 4 * (1 - y) + 2 * x + core
    dn = 4 * (1 - y) + 2 * (1 - x) + core
    other = 4 * y + 2 * x + (1 - core)
    oxn = 4 * y + 2 * (1 - x) + (1 - core)
    oyn = 4 * (1 - y) + 2 * x + (1 - core)
    odn = 4 * (1 - y) + 2 * (1 - x) + (1 - core)
    kt = _ktiles()

    def rows(dev, part=0, size=BLK):
        return pl.ds(pl.multiple_of(dev * BLK + part * HALF, 32), size)

    def remote(kind, n, sl, dev):
        piece = bbuf.at[n, sl]
        return pltpu.make_async_remote_copy(
            src_ref=piece, dst_ref=piece, send_sem=ssem.at[kind, n], recv_sem=rsem.at[kind, n],
            device_id=(dev,), device_id_type=MESH,
        )

    send = {
        0: lambda n: remote(0, n, rows(me), xn),
        1: lambda n: remote(1, n, rows(me), yn),
        2: lambda n: remote(2, n, rows(xn, 0, HALF), yn),
        3: lambda n: remote(3, n, rows(yn, 1, HALF), xn),
        4: lambda n: remote(4, n, rows(xn), other),
        5: lambda n: remote(5, n, rows(yn), other),
        6: lambda n: remote(6, n, rows(dn), other),
    }
    recv = {
        0: lambda n: remote(0, n, rows(xn), xn),
        1: lambda n: remote(1, n, rows(yn), yn),
        2: lambda n: remote(2, n, rows(dn, 0, HALF), yn),
        3: lambda n: remote(3, n, rows(dn, 1, HALF), xn),
        4: lambda n: remote(4, n, rows(oxn), other),
        5: lambda n: remote(5, n, rows(oyn), other),
        6: lambda n: remote(6, n, rows(odn), other),
    }

    def pair(part, dev):
        lo, size = ((0, 1), (1, 2), (3, PANELS - 3))[part]
        piece = bbuf.at[pl.ds(lo, size), rows(dev)]
        return pltpu.make_async_remote_copy(
            src_ref=piece, dst_ref=piece, send_sem=psem.at[0, part], recv_sem=psem.at[1, part],
            device_id=(other,), device_id_type=MESH,
        )

    def aload(i):
        cols = pl.ds(pl.multiple_of(kt[i] * KT, KT), KT)
        return pltpu.make_async_copy(a_ref.at[:, cols], abuf.at[i], asem.at[i - 2])

    def aload_half(i, t):
        cols = pl.ds(pl.multiple_of(kt[i] * KT, KT), KT)
        part = pl.ds(t * TRIP, TRIP)
        return pltpu.make_async_copy(a_ref.at[part, cols], abuf.at[i, part], asem.at[8 + 2 * t + i])

    def bload(n):
        return pltpu.make_async_copy(b_ref.at[:, pl.ds(n * PW, PW)], bbuf.at[n, rows(me)], bsem.at[n])

    def arrived(n):
        recv[0](n).wait_recv()
        recv[1](n).wait_recv()
        for kind in (2, 3, 4, 5):
            send[kind](n).start()

    def ahead(n):
        send[0](n).start()
        send[1](n).start()

    def diagonal(n):
        recv[2](n).wait_recv()
        recv[3](n).wait_recv()
        send[6](n).start()

    def service1(n, depth=2):
        arrived(n)
        ahead(n + depth)

    def xy_ready(n):
        recv[4](n).wait_recv()
        recv[5](n).wait_recv()

    def d_ready(n):
        recv[6](n).wait_recv()

    def product(n, row, poss):
        total = None
        for i in poss:
            left = abuf[i, pl.ds(pl.multiple_of(row, SLAB), SLAB), :]
            right = bbuf[n, pl.ds(pl.multiple_of(kt[i] * KT, KT), KT), :]
            part = jnp.dot(left, right, preferred_element_type=F32)
            total = part if total is None else total + part
        return total

    def out_copy(g, panel, t):
        return pltpu.make_async_copy(
            stage.at[g % 4], c1_ref.at[panel, pl.ds(pl.multiple_of(t * TRIP, TRIP), TRIP)], osem.at[g % 4]
        )

    def keep(n, poss, slot, halves, add=False):
        for t in halves:
            for s in range(3):
                row = t * TRIP + s * SLAB
                at = pl.ds(pl.multiple_of(row, SLAB), SLAB)
                value = product(n, row, poss)
                psum[slot, at, :] = psum[slot, at, :] + value if add else value

    def final(n, poss, slot, halves, wait):
        if wait:
            for t in halves:
                out_copy(2 * n + t, 0, 0).wait()
        for t in halves:
            for s in range(3):
                row = t * TRIP + s * SLAB
                value = product(n, row, poss)
                if slot is not None:
                    value = psum[slot, pl.ds(pl.multiple_of(row, SLAB), SLAB), :] + value
                stage[(2 * n + t) % 4, s * SLAB : (s + 1) * SLAB, :] = value.astype(BF16)
        for t in halves:
            out_copy(2 * n + t, n, t).start()

    def split(body, between):
        def trip(t, _):
            pl.when(t == 1)(between)
            body(t)
            return 0

        lax.fori_loop(0, 2, trip, 0)

    for n in range(PANELS):
        bload(n).start()
    for t in range(2):
        for i in range(2):
            aload_half(i, t).start()
    barrier = pltpu.get_barrier_semaphore()
    for dev in (other, xn, yn):
        pl.semaphore_signal(barrier, inc=1, device_id=(dev,), device_id_type=MESH)
    pl.semaphore_wait(barrier, 3)
    bload(0).wait()
    pair(0, me).start()
    ahead(0)
    bload(1).wait()
    bload(2).wait()
    ahead(1)
    pair(1, me).start()
    for n in range(3, PANELS):
        bload(n).wait()
    pair(2, me).start()

    own, mid, far = [0, 1], [2, 3, 4, 5, 6], [7, 8, 9]
    both = (0, 1)
    pair(0, other).wait_recv()
    for t in range(2):
        for i in range(2):
            aload_half(i, t).wait()
        if t == 1:
            for i in range(2, 10):
                aload(i).start()
        keep(0, own, 0, (t,))
    pair(1, other).wait_recv()
    keep(1, own, 1, both)
    service1(0)
    for i in range(2, 7):
        aload(i).wait()
    xy_ready(0)
    split(lambda t: keep(0, mid, 0, (t,), True), lambda: service1(1))
    diagonal(0)
    xy_ready(1)
    keep(1, mid, 1, both, True)
    service1(2)
    for i in range(7, 10):
        aload(i).wait()
    d_ready(0)
    final(0, far, 0, both, False)
    diagonal(1)
    xy_ready(2)
    split(lambda t: keep(2, own + mid, 0, (t,)), lambda: service1(3))
    diagonal(2)
    d_ready(1)
    final(1, far, 1, both, False)
    service1(4)
    d_ready(2)
    split(lambda t: final(2, far, 0, (t,), True), lambda: diagonal(3))
    pair(2, other).wait_recv()

    def full_half(u, _):
        n, t = 3 + u // 2, u % 2

        @pl.when(t == 0)
        def _():
            xy_ready(n)
            d_ready(n)

        @pl.when((u >= 1) & (u <= 3))
        def _():
            service1(4 + u)

        @pl.when((u == 5) | (u == 6))
        def _():
            arrived(3 + u)

        @pl.when(u == 1)
        def _():
            diagonal(4)

        @pl.when((u >= 3) & (u <= 5))
        def _():
            diagonal(2 + u)

        @pl.when(u == 7)
        def _():
            diagonal(8)
            diagonal(9)

        final(n, own + mid + far, None, (t,), True)
        return 0

    lax.fori_loop(0, 2 * (FIRST - 3), full_half, 0)
    for n in range(FIRST, PANELS):
        xy_ready(n)
        d_ready(n)
    for kind in range(7):
        for n in range(PANELS):
            send[kind](n).wait_send()
    for part in range(3):
        pair(part, me).wait_send()
    for g in range(4):
        out_copy(g, 0, 0).wait()


def _kernel2(abuf, bbuf, c1_ref, c_ref, stage, move, osem, lsem, wsem, *accs):
    mxu = Mxu(accs, abuf, bbuf)
    trips = (PANELS - FIRST) * SLABS // 2
    poss = list(range(10))

    def load(u):
        return pltpu.make_async_copy(c1_ref.at[u], move.at[u % 4], lsem.at[u % 4])

    def store(u):
        cols = pl.ds(pl.multiple_of(u * PW, PW), PW)
        return pltpu.make_async_copy(move.at[u % 4], c_ref.at[:, cols], wsem.at[u % 4])

    def out_copy(tau):
        panel = FIRST + tau // SLABS
        return pltpu.make_async_copy(
            stage.at[tau % 8],
            c_ref.at[
                pl.ds(pl.multiple_of((tau % SLABS) * SLAB, SLAB), SLAB), pl.ds(pl.multiple_of(panel * PW, PW), PW)
            ],
            osem.at[tau % 8],
        )

    load(0).start()
    mxu.clear()
    mxu.push(FIRST, 0, 0)

    def trip(u, _):
        @pl.when((u >= 1) & (u <= FIRST))
        def _():
            load(u - 1).wait()
            store(u - 1).start()

            @pl.when(u < FIRST)
            def _():
                @pl.when(u >= 4)
                def _():
                    store(u - 4).wait()

                load(u).start()

        @pl.when(u >= 4)
        def _():
            out_copy(2 * u - 8).wait()
            out_copy(2 * u - 7).wait()

        reg = 0
        for j in range(2):
            tau = 2 * u + j
            panel = FIRST + tau // SLABS
            nextpanel = FIRST + ((tau + 1) // SLABS) % (PANELS - FIRST)

            def emit(row, value, slot=(tau + 7) % 8):
                stage[slot, pl.ds(row, PART), :] = value.astype(BF16)

            reg = mxu.tile(j, tau % SLABS, panel, nextpanel, poss, reg, emit)

        @pl.when(u > 0)
        def _():
            out_copy(2 * u - 1).start()

        out_copy(2 * u).start()
        return 0

    lax.fori_loop(0, trips, trip, 0)
    last = 2 * trips - 1

    def emit(row, value):
        stage[last % 8, pl.ds(row, PART), :] = value.astype(BF16)

    mxu.drain(1, emit)
    out_copy(last).start()
    mxu.drop(0)
    for u in range(FIRST - 4, FIRST):
        store(u).wait()
    for tau in range(2 * trips - 8, last + 1):
        out_copy(tau).wait()


def _with_accs(kernel):
    def run(*refs):
        specs = [pltpu.ACC(q)((PART, PW), F32) for _ in range(2) for q in range(2) for _ in range(4)]
        pl.run_scoped(lambda *accs: kernel(*refs, *accs), *specs)

    return run


def _local(a, b):
    any_ = pl.BlockSpec(memory_space=pltpu.HBM)
    vmem = pl.BlockSpec(memory_space=pltpu.VMEM)
    dma = pltpu.SemaphoreType.DMA
    abuf, bbuf, c1 = pl.pallas_call(
        _kernel1,
        out_shape=(
            pltpu.VMEM((10, ROWS, KT), BF16),
            pltpu.VMEM((PANELS, DEPTH, PW), BF16),
            pltpu.HBM((FIRST, ROWS, PW), BF16),
        ),
        in_specs=[any_, any_],
        out_specs=(vmem, vmem, any_),
        scratch_shapes=[
            pltpu.VMEM((2, ROWS, PW), F32),
            pltpu.VMEM((4, TRIP, PW), BF16),
            dma((12,)),
            dma((PANELS,)),
            dma((4,)),
            dma((7, PANELS)),
            dma((7, PANELS)),
            dma((2, 3)),
        ],
        compiler_params=pltpu.CompilerParams(
            collective_id=0, has_side_effects=True, vmem_limit_bytes=GRANT
        ),
    )(a, b)
    abuf = pltpu.with_memory_space_constraint(abuf, pltpu.VMEM)
    bbuf = pltpu.with_memory_space_constraint(bbuf, pltpu.VMEM)
    c1 = pltpu.with_memory_space_constraint(c1, pltpu.HBM)
    return pl.pallas_call(
        _with_accs(_kernel2),
        out_shape=jax.ShapeDtypeStruct((ROWS, DEPTH), BF16),
        in_specs=[vmem, vmem, any_],
        out_specs=any_,
        scratch_shapes=[
            pltpu.VMEM((8, SLAB, PW), BF16),
            pltpu.VMEM((4, ROWS, PW), BF16),
            dma((8,)),
            dma((4,)),
            dma((4,)),
        ],
        compiler_params=pltpu.CompilerParams(vmem_limit_bytes=GRANT),
    )(abuf, bbuf, c1)


def solution(mesh):
    spec = P("fsdp", None)
    return jax.shard_map(_local, mesh=mesh, in_specs=(spec, spec), out_specs=spec, check_vma=False)
```

```python
import jax
import jax.numpy as jnp
from jax import lax
from jax.experimental import pallas as pl
from jax.experimental.pallas import tpu as pltpu
from jax.sharding import PartitionSpec as P

MESH = pl.DeviceIdType.MESH
BF16 = jnp.bfloat16
F32 = jnp.float32
ROWS = 6144
SLAB = 1024
SLABS = ROWS // SLAB
TRIP = 3 * SLAB
DEPTH = 2560
KT = 256
PW = 256
PANELS = 10
BLK = 320
HALF = BLK // 2
PART = 128
FIRST = 7
GRANT = int(21.4 * 2**20)


def _place():
    me = lax.axis_index("fsdp")
    core = me % 2
    x = (me // 2) % 2
    y = me // 4
    return me, core, x, y


def _ktiles():
    _, _, x, y = _place()
    own, other = 5 * y, 5 * (1 - y)
    return (
        [own + 3 * x + i for i in range(2)]
        + [own + 2 * (1 - x) + i for i in range(3)]
        + [other + 3 * x + i for i in range(2)]
        + [other + 2 * (1 - x) + i for i in range(3)]
    )


class Mxu:
    def __init__(self, accs, abuf, bbuf):
        self.accs, self.abuf, self.bbuf = accs, abuf, bbuf
        self.kt = _ktiles()

    def acc(self, rng, q, p):
        return self.accs[(rng * 2 + q) * 4 + p]

    def push(self, panel, i, reg):
        rows = pl.ds(pl.multiple_of(self.kt[i] * KT, KT), KT)
        for q in range(2):
            pltpu.matmul_push_rhs(self.bbuf[panel, rows, :], staging_register=reg, mxu_index=q)

    def drop(self, reg):
        zero = jnp.zeros((PART, KT), BF16)
        for q in range(2):
            pltpu.matmul_acc_lhs(self.acc(0, q, 0), zero, load_staged_rhs=reg)

    def clear(self):
        for r in self.accs:
            pltpu.matmul_pop(r)

    def tile(self, rng, slab, panel, nextpanel, poss, start_reg, emit):
        n = len(poss)
        reg = start_reg
        pieces = [(p, q) for p in range(4) for q in range(2)]
        slots = 4 if n > 4 else n - 1
        per = -(-len(pieces) // max(slots, 1))
        for k, i in enumerate(poss):
            for q in range(2):
                for p in range(4):
                    rows = pl.ds(pl.multiple_of(slab * SLAB + q * 512 + p * PART, PART), PART)
                    pltpu.matmul_acc_lhs(
                        self.acc(rng, q, p), self.abuf[rows, i * KT : (i + 1) * KT], load_staged_rhs=reg if p == 0 else None
                    )
            reg = 1 - reg
            if k < n - 1:
                self.push(panel, poss[k + 1], reg)
            else:
                self.push(nextpanel, poss[0], reg)
            if k >= 1:
                for p, q in pieces[(k - 1) * per : k * per]:
                    emit(q * 512 + p * PART, pltpu.matmul_pop(self.acc(1 - rng, q, p)))
        return reg

    def drain(self, rng, emit):
        for p in range(4):
            for q in range(2):
                emit(q * 512 + p * PART, pltpu.matmul_pop(self.acc(rng, q, p)))


def _kernel1(a_ref, b_ref, abuf, bbuf, c1_ref, psum, stage, asem, bsem, osem, ssem, rsem, psem):
    me, core, x, y = _place()
    xn = 4 * y + 2 * (1 - x) + core
    yn = 4 * (1 - y) + 2 * x + core
    dn = 4 * (1 - y) + 2 * (1 - x) + core
    other = 4 * y + 2 * x + (1 - core)
    oxn = 4 * y + 2 * (1 - x) + (1 - core)
    oyn = 4 * (1 - y) + 2 * x + (1 - core)
    odn = 4 * (1 - y) + 2 * (1 - x) + (1 - core)
    kt = _ktiles()

    def rows(dev, part=0, size=BLK):
        return pl.ds(pl.multiple_of(dev * BLK + part * HALF, 32), size)

    def remote(kind, n, sl, dev):
        piece = bbuf.at[n, sl]
        return pltpu.make_async_remote_copy(
            src_ref=piece, dst_ref=piece, send_sem=ssem.at[kind, n], recv_sem=rsem.at[kind, n],
            device_id=(dev,), device_id_type=MESH,
        )

    send = {
        0: lambda n: remote(0, n, rows(me), xn),
        1: lambda n: remote(1, n, rows(me), yn),
        2: lambda n: remote(2, n, rows(xn, 0, HALF), yn),
        3: lambda n: remote(3, n, rows(yn, 1, HALF), xn),
        4: lambda n: remote(4, n, rows(xn), other),
        5: lambda n: remote(5, n, rows(yn), other),
        6: lambda n: remote(6, n, rows(dn), other),
    }
    recv = {
        0: lambda n: remote(0, n, rows(xn), xn),
        1: lambda n: remote(1, n, rows(yn), yn),
        2: lambda n: remote(2, n, rows(dn, 0, HALF), yn),
        3: lambda n: remote(3, n, rows(dn, 1, HALF), xn),
        4: lambda n: remote(4, n, rows(oxn), other),
        5: lambda n: remote(5, n, rows(oyn), other),
        6: lambda n: remote(6, n, rows(odn), other),
    }

    def pair(part, dev):
        lo, size = ((0, 1), (1, 2), (3, PANELS - 3))[part]
        piece = bbuf.at[pl.ds(lo, size), rows(dev)]
        return pltpu.make_async_remote_copy(
            src_ref=piece, dst_ref=piece, send_sem=psem.at[0, part], recv_sem=psem.at[1, part],
            device_id=(other,), device_id_type=MESH,
        )

    groups = ((0, 2), (2, 3), (5, 2), (7, 3))

    def aload(i, t):
        first, count = groups[i]
        cols = pl.ds(pl.multiple_of(kt[first] * KT, KT), count * KT)
        part = pl.ds(pl.multiple_of(t * TRIP, TRIP), TRIP)
        return pltpu.make_async_copy(
            a_ref.at[part, cols], abuf.at[part, pl.ds(first * KT, count * KT)], asem.at[i, t]
        )

    def bload(n):
        return pltpu.make_async_copy(b_ref.at[:, pl.ds(n * PW, PW)], bbuf.at[n, rows(me)], bsem.at[n])

    def arrived(n):
        recv[0](n).wait_recv()
        recv[1](n).wait_recv()
        for kind in (2, 3, 4, 5):
            send[kind](n).start()

    def ahead(n):
        send[0](n).start()
        send[1](n).start()

    def diagonal(n):
        recv[2](n).wait_recv()
        recv[3](n).wait_recv()
        send[6](n).start()

    def service1(n, depth=2):
        arrived(n)
        ahead(n + depth)

    def xy_ready(n):
        recv[4](n).wait_recv()
        recv[5](n).wait_recv()

    def d_ready(n):
        recv[6](n).wait_recv()

    def product(n, row, poss):
        total = None
        for i in poss:
            left = abuf[pl.ds(pl.multiple_of(row, SLAB), SLAB), i * KT : (i + 1) * KT]
            right = bbuf[n, pl.ds(pl.multiple_of(kt[i] * KT, KT), KT), :]
            part = jnp.dot(left, right, preferred_element_type=F32)
            total = part if total is None else total + part
        return total

    def out_copy(g, panel, t):
        return pltpu.make_async_copy(
            stage.at[g % 2], c1_ref.at[panel, pl.ds(pl.multiple_of(t * TRIP, TRIP), TRIP)], osem.at[g % 2]
        )

    def held(slot, row):
        return pl.ds(pl.multiple_of(slot * ROWS + row, SLAB), SLAB)

    def scoped(fn):
        pl.when(me >= 0)(fn)

    def keep(n, poss, slot, halves, add=False):
        for t in halves:
            for s in range(3):
                row = t * TRIP + s * SLAB
                at = held(slot, row)
                value = product(n, row, poss)
                psum[at, :] = psum[at, :] + value if add else value

    def final(n, poss, slot, halves, wait):
        if wait:
            for t in halves:
                out_copy(2 * n + t, 0, 0).wait()
        for t in halves:
            for s in range(3):
                row = t * TRIP + s * SLAB
                value = product(n, row, poss)
                if slot is not None:
                    value = psum[held(slot, row), :] + value
                stage[(2 * n + t) % 2, s * SLAB : (s + 1) * SLAB, :] = value.astype(BF16)
        for t in halves:
            out_copy(2 * n + t, n, t).start()

    def split(body, between):
        def trip(t, _):
            pl.when(t == 1)(between)
            body(t)
            return 0

        lax.fori_loop(0, 2, trip, 0)

    for n in range(PANELS):
        bload(n).start()
    for t in range(2):
        aload(0, t).start()
    barrier = pltpu.get_barrier_semaphore()
    for dev in (other, xn, yn):
        pl.semaphore_signal(barrier, inc=1, device_id=(dev,), device_id_type=MESH)
    pl.semaphore_wait(barrier, 3)
    bload(0).wait()
    pair(0, me).start()
    ahead(0)
    bload(1).wait()
    bload(2).wait()
    ahead(1)
    pair(1, me).start()
    for n in range(3, PANELS):
        bload(n).wait()
    pair(2, me).start()

    own, mid, far = [0, 1], [2, 3, 4, 5, 6], [7, 8, 9]
    both = (0, 1)
    pair(0, other).wait_recv()
    for t in range(2):
        aload(0, t).wait()
        for h in both:
            for i in (1, 2) if t == 0 else (3,):
                aload(i, h).start()
        keep(0, own, 0, (t,))
    pair(1, other).wait_recv()
    keep(1, own, 1, both)
    service1(0)
    scoped(lambda: keep(2, own, 2, (0,)))
    xy_ready(0)

    def first_mid(t):
        aload(1, t).wait()
        aload(2, t).wait()
        keep(0, mid, 0, (t,), True)

    split(first_mid, lambda: service1(1))
    diagonal(0)
    xy_ready(1)
    keep(1, mid, 1, both, True)
    service1(2)
    for h in both:
        aload(3, h).wait()
    d_ready(0)
    final(0, far, 0, both, False)
    diagonal(1)
    xy_ready(2)
    scoped(lambda: keep(2, mid, 2, (0,), True))
    service1(3)
    d_ready(1)
    final(1, far, 1, both, True)
    diagonal(2)
    service1(4)
    scoped(lambda: keep(2, own + mid, 0, (1,)))
    d_ready(2)
    scoped(lambda: final(2, far, 2, (0,), True))
    diagonal(3)
    scoped(lambda: final(2, far, 0, (1,), True))
    pair(2, other).wait_recv()

    def full_half(u, _):
        n, t = 3 + u // 2, u % 2

        @pl.when(t == 0)
        def _():
            xy_ready(n)
            d_ready(n)

        @pl.when((u >= 1) & (u <= 3))
        def _():
            service1(4 + u)

        @pl.when((u == 5) | (u == 6))
        def _():
            arrived(3 + u)

        @pl.when(u == 1)
        def _():
            diagonal(4)

        @pl.when((u >= 3) & (u <= 5))
        def _():
            diagonal(2 + u)

        @pl.when(u == 7)
        def _():
            diagonal(8)
            diagonal(9)

        final(n, own + mid + far, None, (t,), True)
        return 0

    lax.fori_loop(0, 2 * (FIRST - 3), full_half, 0)
    for n in range(FIRST, PANELS):
        xy_ready(n)
        d_ready(n)
    for kind in range(7):
        for n in range(PANELS):
            send[kind](n).wait_send()
    for part in range(3):
        pair(part, me).wait_send()
    for g in range(2):
        out_copy(g, 0, 0).wait()


def _kernel2(abuf, bbuf, c1_ref, c_ref, stage, move, osem, lsem, wsem, *accs):
    mxu = Mxu(accs, abuf, bbuf)
    trips = (PANELS - FIRST) * SLABS // 2
    poss = list(range(10))

    def load(u):
        return pltpu.make_async_copy(c1_ref.at[u], move.at[u % 4], lsem.at[u % 4])

    def store(u):
        cols = pl.ds(pl.multiple_of(u * PW, PW), PW)
        return pltpu.make_async_copy(move.at[u % 4], c_ref.at[:, cols], wsem.at[u % 4])

    def out_copy(tau):
        panel = FIRST + tau // SLABS
        return pltpu.make_async_copy(
            stage.at[tau % 8],
            c_ref.at[
                pl.ds(pl.multiple_of((tau % SLABS) * SLAB, SLAB), SLAB), pl.ds(pl.multiple_of(panel * PW, PW), PW)
            ],
            osem.at[tau % 8],
        )

    load(0).start()
    mxu.clear()
    mxu.push(FIRST, 0, 0)

    def trip(u, _):
        @pl.when((u >= 1) & (u <= FIRST))
        def _():
            load(u - 1).wait()
            store(u - 1).start()

            @pl.when(u < FIRST)
            def _():
                @pl.when(u >= 4)
                def _():
                    store(u - 4).wait()

                load(u).start()

        @pl.when(u >= 4)
        def _():
            out_copy(2 * u - 8).wait()
            out_copy(2 * u - 7).wait()

        reg = 0
        for j in range(2):
            tau = 2 * u + j
            panel = FIRST + tau // SLABS
            nextpanel = FIRST + ((tau + 1) // SLABS) % (PANELS - FIRST)

            def emit(row, value, slot=(tau + 7) % 8):
                stage[slot, pl.ds(row, PART), :] = value.astype(BF16)

            reg = mxu.tile(j, tau % SLABS, panel, nextpanel, poss, reg, emit)

        @pl.when(u > 0)
        def _():
            out_copy(2 * u - 1).start()

        out_copy(2 * u).start()
        return 0

    lax.fori_loop(0, trips, trip, 0)
    last = 2 * trips - 1

    def emit(row, value):
        stage[last % 8, pl.ds(row, PART), :] = value.astype(BF16)

    mxu.drain(1, emit)
    out_copy(last).start()
    mxu.drop(0)
    for u in range(FIRST - 4, FIRST):
        store(u).wait()
    for tau in range(2 * trips - 8, last + 1):
        out_copy(tau).wait()


def _with_accs(kernel):
    def run(*refs):
        specs = [pltpu.ACC(q)((PART, PW), F32) for _ in range(2) for q in range(2) for _ in range(4)]
        pl.run_scoped(lambda *accs: kernel(*refs, *accs), *specs)

    return run


def _local(a, b):
    any_ = pl.BlockSpec(memory_space=pltpu.HBM)
    vmem = pl.BlockSpec(memory_space=pltpu.VMEM)
    dma = pltpu.SemaphoreType.DMA
    abuf, bbuf, c1 = pl.pallas_call(
        _kernel1,
        out_shape=(
            pltpu.VMEM((ROWS, DEPTH), BF16),
            pltpu.VMEM((PANELS, DEPTH, PW), BF16),
            pltpu.HBM((FIRST, ROWS, PW), BF16),
        ),
        in_specs=[any_, any_],
        out_specs=(vmem, vmem, any_),
        scratch_shapes=[
            pltpu.VMEM((2 * ROWS + TRIP, PW), F32),
            pltpu.VMEM((2, TRIP, PW), BF16),
            dma((4, 2)),
            dma((PANELS,)),
            dma((2,)),
            dma((7, PANELS)),
            dma((7, PANELS)),
            dma((2, 3)),
        ],
        compiler_params=pltpu.CompilerParams(
            collective_id=0, has_side_effects=True, vmem_limit_bytes=GRANT
        ),
    )(a, b)
    abuf = pltpu.with_memory_space_constraint(abuf, pltpu.VMEM)
    bbuf = pltpu.with_memory_space_constraint(bbuf, pltpu.VMEM)
    c1 = pltpu.with_memory_space_constraint(c1, pltpu.HBM)
    return pl.pallas_call(
        _with_accs(_kernel2),
        out_shape=jax.ShapeDtypeStruct((ROWS, DEPTH), BF16),
        in_specs=[vmem, vmem, any_],
        out_specs=any_,
        scratch_shapes=[
            pltpu.VMEM((8, SLAB, PW), BF16),
            pltpu.VMEM((4, ROWS, PW), BF16),
            dma((8,)),
            dma((4,)),
            dma((4,)),
        ],
        compiler_params=pltpu.CompilerParams(vmem_limit_bytes=GRANT),
    )(abuf, bbuf, c1)


def solution(mesh):
    spec = P("fsdp", None)
    return jax.shard_map(_local, mesh=mesh, in_specs=(spec, spec), out_specs=spec, check_vma=False)
```

```python
import jax
import jax.numpy as jnp
from jax import lax
from jax.experimental import pallas as pl
from jax.experimental.pallas import tpu as pltpu
from jax.sharding import PartitionSpec as P

MESH = pl.DeviceIdType.MESH
BF16 = jnp.bfloat16
F32 = jnp.float32
ROWS = 6144
SLAB = 1024
SLABS = ROWS // SLAB
TRIP = 3 * SLAB
DEPTH = 2560
KT = 256
PW = 256
PANELS = 10
BLK = 320
HALF = BLK // 2
PART = 128
FIRST = 7
GRANT = int(21.4 * 2**20)


def _place():
    me = lax.axis_index("fsdp")
    core = me % 2
    x = (me // 2) % 2
    y = me // 4
    return me, core, x, y


def _ktiles():
    _, _, x, y = _place()
    own, other = 5 * y, 5 * (1 - y)
    return (
        [own + 3 * x + i for i in range(2)]
        + [own + 2 * (1 - x) + i for i in range(3)]
        + [other + 3 * x + i for i in range(2)]
        + [other + 2 * (1 - x) + i for i in range(3)]
    )


class Mxu:
    def __init__(self, accs, abuf, bbuf):
        self.accs, self.abuf, self.bbuf = accs, abuf, bbuf
        self.kt = _ktiles()

    def acc(self, rng, q, p):
        return self.accs[(rng * 2 + q) * 4 + p]

    def push(self, panel, i, reg):
        rows = pl.ds(pl.multiple_of(self.kt[i] * KT, KT), KT)
        for q in range(2):
            pltpu.matmul_push_rhs(self.bbuf[panel, rows, :], staging_register=reg, mxu_index=q)

    def drop(self, reg):
        zero = jnp.zeros((PART, KT), BF16)
        for q in range(2):
            pltpu.matmul_acc_lhs(self.acc(0, q, 0), zero, load_staged_rhs=reg)

    def clear(self):
        for r in self.accs:
            pltpu.matmul_pop(r)

    def tile(self, rng, slab, panel, nextpanel, poss, start_reg, emit):
        n = len(poss)
        reg = start_reg
        pieces = [(p, q) for p in range(4) for q in range(2)]
        slots = 4 if n > 4 else n - 1
        per = -(-len(pieces) // max(slots, 1))
        for k, i in enumerate(poss):
            for q in range(2):
                for p in range(4):
                    rows = pl.ds(pl.multiple_of(slab * SLAB + q * 512 + p * PART, PART), PART)
                    pltpu.matmul_acc_lhs(
                        self.acc(rng, q, p), self.abuf[rows, i * KT : (i + 1) * KT], load_staged_rhs=reg if p == 0 else None
                    )
            reg = 1 - reg
            if k < n - 1:
                self.push(panel, poss[k + 1], reg)
            else:
                self.push(nextpanel, poss[0], reg)
            if k >= 1:
                for p, q in pieces[(k - 1) * per : k * per]:
                    emit(q * 512 + p * PART, pltpu.matmul_pop(self.acc(1 - rng, q, p)))
        return reg

    def drain(self, rng, emit):
        for p in range(4):
            for q in range(2):
                emit(q * 512 + p * PART, pltpu.matmul_pop(self.acc(rng, q, p)))


def _kernel1(a_ref, b_ref, abuf, bbuf, c1_ref, psum, stage, asem, bsem, osem, ssem, rsem, psem):
    me, core, x, y = _place()
    xn = 4 * y + 2 * (1 - x) + core
    yn = 4 * (1 - y) + 2 * x + core
    dn = 4 * (1 - y) + 2 * (1 - x) + core
    other = 4 * y + 2 * x + (1 - core)
    oxn = 4 * y + 2 * (1 - x) + (1 - core)
    oyn = 4 * (1 - y) + 2 * x + (1 - core)
    odn = 4 * (1 - y) + 2 * (1 - x) + (1 - core)
    kt = _ktiles()

    def rows(dev, part=0, size=BLK):
        return pl.ds(pl.multiple_of(dev * BLK + part * HALF, 32), size)

    def remote(kind, n, sl, dev):
        piece = bbuf.at[n, sl]
        return pltpu.make_async_remote_copy(
            src_ref=piece, dst_ref=piece, send_sem=ssem.at[kind, n], recv_sem=rsem.at[kind, n],
            device_id=(dev,), device_id_type=MESH,
        )

    send = {
        0: lambda n: remote(0, n, rows(me), xn),
        1: lambda n: remote(1, n, rows(me), yn),
        2: lambda n: remote(2, n, rows(xn, 0, HALF), yn),
        3: lambda n: remote(3, n, rows(yn, 1, HALF), xn),
        4: lambda n: remote(4, n, rows(xn), other),
        5: lambda n: remote(5, n, rows(yn), other),
        6: lambda n: remote(6, n, rows(dn), other),
    }
    recv = {
        0: lambda n: remote(0, n, rows(xn), xn),
        1: lambda n: remote(1, n, rows(yn), yn),
        2: lambda n: remote(2, n, rows(dn, 0, HALF), yn),
        3: lambda n: remote(3, n, rows(dn, 1, HALF), xn),
        4: lambda n: remote(4, n, rows(oxn), other),
        5: lambda n: remote(5, n, rows(oyn), other),
        6: lambda n: remote(6, n, rows(odn), other),
    }

    def pair(part, dev):
        lo, size = ((0, 1), (1, 2), (3, PANELS - 3))[part]
        piece = bbuf.at[pl.ds(lo, size), rows(dev)]
        return pltpu.make_async_remote_copy(
            src_ref=piece, dst_ref=piece, send_sem=psem.at[0, part], recv_sem=psem.at[1, part],
            device_id=(other,), device_id_type=MESH,
        )

    groups = ((0, 2), (2, 3), (5, 2), (7, 3))

    def aload(i, t):
        first, count = groups[i]
        cols = pl.ds(pl.multiple_of(kt[first] * KT, KT), count * KT)
        part = pl.ds(pl.multiple_of(t * TRIP, TRIP), TRIP)
        return pltpu.make_async_copy(
            a_ref.at[part, cols], abuf.at[part, pl.ds(first * KT, count * KT)], asem.at[i, t]
        )

    def bload(n):
        return pltpu.make_async_copy(b_ref.at[:, pl.ds(n * PW, PW)], bbuf.at[n, rows(me)], bsem.at[n])

    def arrived(n):
        recv[0](n).wait_recv()
        recv[1](n).wait_recv()
        for kind in (2, 3, 4, 5):
            send[kind](n).start()

    def ahead(n):
        send[0](n).start()
        send[1](n).start()

    def diagonal(n):
        recv[2](n).wait_recv()
        recv[3](n).wait_recv()
        send[6](n).start()

    def service1(n, depth=2):
        arrived(n)
        ahead(n + depth)

    def xy_ready(n):
        recv[4](n).wait_recv()
        recv[5](n).wait_recv()

    def d_ready(n):
        recv[6](n).wait_recv()

    def product(n, row, poss):
        total = None
        for i in poss:
            left = abuf[pl.ds(pl.multiple_of(row, SLAB), SLAB), i * KT : (i + 1) * KT]
            right = bbuf[n, pl.ds(pl.multiple_of(kt[i] * KT, KT), KT), :]
            part = jnp.dot(left, right, preferred_element_type=F32)
            total = part if total is None else total + part
        return total

    def out_copy(g, panel, t):
        return pltpu.make_async_copy(
            stage.at[g % 2], c1_ref.at[panel, pl.ds(pl.multiple_of(t * TRIP, TRIP), TRIP)], osem.at[g % 2]
        )

    def held(slot, row):
        return pl.ds(pl.multiple_of(slot * ROWS + row, SLAB), SLAB)

    def scoped(fn):
        pl.when(me >= 0)(fn)

    def keep(n, poss, slot, halves, add=False):
        for t in halves:
            for s in range(3):
                row = t * TRIP + s * SLAB
                at = held(slot, row)
                value = product(n, row, poss)
                psum[at, :] = psum[at, :] + value if add else value

    def final(n, poss, slot, halves, wait):
        if wait:
            for t in halves:
                out_copy(2 * n + t, 0, 0).wait()
        for t in halves:
            for s in range(3):
                row = t * TRIP + s * SLAB
                value = product(n, row, poss)
                if slot is not None:
                    value = psum[held(slot, row), :] + value
                stage[(2 * n + t) % 2, s * SLAB : (s + 1) * SLAB, :] = value.astype(BF16)
        for t in halves:
            out_copy(2 * n + t, n, t).start()

    def split(body, between):
        def trip(t, _):
            pl.when(t == 1)(between)
            body(t)
            return 0

        lax.fori_loop(0, 2, trip, 0)

    for n in range(PANELS):
        bload(n).start()
    for t in range(2):
        aload(0, t).start()
    barrier = pltpu.get_barrier_semaphore()
    for dev in (other, xn, yn):
        pl.semaphore_signal(barrier, inc=1, device_id=(dev,), device_id_type=MESH)
    pl.semaphore_wait(barrier, 3)
    bload(0).wait()
    pair(0, me).start()
    ahead(0)
    bload(1).wait()
    bload(2).wait()
    ahead(1)
    pair(1, me).start()
    for n in range(3, PANELS):
        bload(n).wait()
    pair(2, me).start()

    own, mid, far = [0, 1], [2, 3, 4, 5, 6], [7, 8, 9]
    both = (0, 1)
    pair(0, other).wait_recv()
    for t in range(2):
        aload(0, t).wait()
        for h in both:
            for i in (1, 2) if t == 0 else (3,):
                aload(i, h).start()
        keep(0, own, 0, (t,))
    pair(1, other).wait_recv()
    keep(1, own, 1, both)
    service1(0)
    scoped(lambda: keep(2, own, 2, (0,)))
    xy_ready(0)

    def first_mid(t):
        aload(1, t).wait()
        aload(2, t).wait()
        keep(0, mid, 0, (t,), True)

    split(first_mid, lambda: service1(1))
    diagonal(0)
    xy_ready(1)
    keep(1, mid, 1, both, True)
    service1(2)
    for h in both:
        aload(3, h).wait()
    d_ready(0)
    final(0, far, 0, both, False)
    diagonal(1)
    xy_ready(2)
    scoped(lambda: keep(2, mid, 2, (0,), True))
    service1(3)
    d_ready(1)
    final(1, far, 1, both, True)
    diagonal(2)
    service1(4)
    ahead(7)
    scoped(lambda: keep(2, own + mid, 0, (1,)))
    d_ready(2)
    scoped(lambda: final(2, far, 2, (0,), True))
    diagonal(3)
    scoped(lambda: final(2, far, 0, (1,), True))
    pair(2, other).wait_recv()

    def full_half(u, _):
        n, t = 3 + u // 2, u % 2

        @pl.when(t == 0)
        def _():
            xy_ready(n)
            d_ready(n)

        @pl.when((u == 1) | (u == 2))
        def _():
            service1(4 + u, 3)

        @pl.when(u == 3)
        def _():
            arrived(7)

        @pl.when((u == 5) | (u == 6))
        def _():
            arrived(3 + u)

        @pl.when(u == 1)
        def _():
            diagonal(4)

        @pl.when((u >= 3) & (u <= 5))
        def _():
            diagonal(2 + u)

        @pl.when(u == 7)
        def _():
            diagonal(8)
            diagonal(9)

        final(n, own + mid + far, None, (t,), True)
        return 0

    lax.fori_loop(0, 2 * (FIRST - 3), full_half, 0)
    for n in range(FIRST, PANELS):
        xy_ready(n)
        d_ready(n)
    for kind in range(7):
        for n in range(PANELS):
            send[kind](n).wait_send()
    for part in range(3):
        pair(part, me).wait_send()
    for g in range(2):
        out_copy(g, 0, 0).wait()


def _kernel2(abuf, bbuf, c1_ref, c_ref, stage, move, osem, lsem, wsem, *accs):
    mxu = Mxu(accs, abuf, bbuf)
    trips = (PANELS - FIRST) * SLABS // 2
    poss = list(range(10))

    def load(u):
        return pltpu.make_async_copy(c1_ref.at[u], move.at[u % 4], lsem.at[u % 4])

    def store(u):
        cols = pl.ds(pl.multiple_of(u * PW, PW), PW)
        return pltpu.make_async_copy(move.at[u % 4], c_ref.at[:, cols], wsem.at[u % 4])

    def out_copy(tau):
        panel = FIRST + tau // SLABS
        return pltpu.make_async_copy(
            stage.at[tau % 8],
            c_ref.at[
                pl.ds(pl.multiple_of((tau % SLABS) * SLAB, SLAB), SLAB), pl.ds(pl.multiple_of(panel * PW, PW), PW)
            ],
            osem.at[tau % 8],
        )

    load(0).start()
    mxu.clear()
    mxu.push(FIRST, 0, 0)

    def trip(u, _):
        @pl.when((u >= 1) & (u <= FIRST))
        def _():
            load(u - 1).wait()
            store(u - 1).start()

            @pl.when(u < FIRST)
            def _():
                @pl.when(u >= 4)
                def _():
                    store(u - 4).wait()

                load(u).start()

        @pl.when(u >= 4)
        def _():
            out_copy(2 * u - 8).wait()
            out_copy(2 * u - 7).wait()

        reg = 0
        for j in range(2):
            tau = 2 * u + j
            panel = FIRST + tau // SLABS
            nextpanel = FIRST + ((tau + 1) // SLABS) % (PANELS - FIRST)

            def emit(row, value, slot=(tau + 7) % 8):
                stage[slot, pl.ds(row, PART), :] = value.astype(BF16)

            reg = mxu.tile(j, tau % SLABS, panel, nextpanel, poss, reg, emit)

        @pl.when(u > 0)
        def _():
            out_copy(2 * u - 1).start()

        out_copy(2 * u).start()
        return 0

    lax.fori_loop(0, trips, trip, 0)
    last = 2 * trips - 1

    def emit(row, value):
        stage[last % 8, pl.ds(row, PART), :] = value.astype(BF16)

    mxu.drain(1, emit)
    out_copy(last).start()
    mxu.drop(0)
    for u in range(FIRST - 4, FIRST):
        store(u).wait()
    for tau in range(2 * trips - 8, last + 1):
        out_copy(tau).wait()


def _with_accs(kernel):
    def run(*refs):
        specs = [pltpu.ACC(q)((PART, PW), F32) for _ in range(2) for q in range(2) for _ in range(4)]
        pl.run_scoped(lambda *accs: kernel(*refs, *accs), *specs)

    return run


def _local(a, b):
    any_ = pl.BlockSpec(memory_space=pltpu.HBM)
    vmem = pl.BlockSpec(memory_space=pltpu.VMEM)
    dma = pltpu.SemaphoreType.DMA
    abuf, bbuf, c1 = pl.pallas_call(
        _kernel1,
        out_shape=(
            pltpu.VMEM((ROWS, DEPTH), BF16),
            pltpu.VMEM((PANELS, DEPTH, PW), BF16),
            pltpu.HBM((FIRST, ROWS, PW), BF16),
        ),
        in_specs=[any_, any_],
        out_specs=(vmem, vmem, any_),
        scratch_shapes=[
            pltpu.VMEM((2 * ROWS + TRIP, PW), F32),
            pltpu.VMEM((2, TRIP, PW), BF16),
            dma((4, 2)),
            dma((PANELS,)),
            dma((2,)),
            dma((7, PANELS)),
            dma((7, PANELS)),
            dma((2, 3)),
        ],
        compiler_params=pltpu.CompilerParams(
            collective_id=0, has_side_effects=True, vmem_limit_bytes=GRANT
        ),
    )(a, b)
    abuf = pltpu.with_memory_space_constraint(abuf, pltpu.VMEM)
    bbuf = pltpu.with_memory_space_constraint(bbuf, pltpu.VMEM)
    c1 = pltpu.with_memory_space_constraint(c1, pltpu.HBM)
    return pl.pallas_call(
        _with_accs(_kernel2),
        out_shape=jax.ShapeDtypeStruct((ROWS, DEPTH), BF16),
        in_specs=[vmem, vmem, any_],
        out_specs=any_,
        scratch_shapes=[
            pltpu.VMEM((8, SLAB, PW), BF16),
            pltpu.VMEM((4, ROWS, PW), BF16),
            dma((8,)),
            dma((4,)),
            dma((4,)),
        ],
        compiler_params=pltpu.CompilerParams(vmem_limit_bytes=GRANT),
    )(abuf, bbuf, c1)


def solution(mesh):
    spec = P("fsdp", None)
    return jax.shard_map(_local, mesh=mesh, in_specs=(spec, spec), out_specs=spec, check_vma=False)
```
